32 devices in a mesh: row: 4 (over y, x), col: 8 (over z, core).
Axes of the slice: x: 2, y: 2, z: 4, core: 2. Of those that a mesh axis runs over, the one named last changes fastest.
Arguments:
- source_blocks: float32 [8192, 24576], P('row', 'col'), may hold values from -6 to 6
Outputs:
- target_blocks: float32 [4096, 49152], P('row', 'col')
- column_sums: float32 [49152], P('col')
- frobenius: float32 [], replicated
The draws below stay inside these ranges and needn't reach their ends.
All inputs are finite; a program needn't handle non-finite values.
Results may differ from the reference program's by a relative error of at most 0.00002.
Values sent between devices are 32-bit elements; how exact they have to be, the bound alone decides.
No kernel may reach another device: no remote copies, remote signals or barrier semaphores. Data moves between devices by JAX's collectives and lax.ppermute only.
A program may use at most 192 MiB of HBM per device.

```python
import math
import jax
import jax.numpy as jnp
from jax import lax

N = 24576
SB = 128
RB = 2
TB = 512
M = 8192
E = 12
N_ROW = 4
N_COL = 8


def strengthened(drawn, own_key, source, target, parts, factor):
    owner, partner = [(jnp.arange(drawn.shape[dim]) // (drawn.shape[dim] // parts)).reshape([-1 if axis == dim else 1 for axis in range(drawn.ndim)]) for dim in (source, target)]
    chosen = jax.random.permutation(own_key, parts)[partner]
    strong = (owner == chosen) | (owner == (partner + parts // 2) % parts)
    return jnp.where(strong, factor * drawn, drawn)


def block_scale(key, shape, cuts, smallest, top_value):
    factor_of, own = 1.0, jax.random.fold_in(key, 6)
    for dim, blocks in cuts:
        steps = jnp.exp(jax.random.uniform(jax.random.fold_in(own, dim), (blocks,), jnp.float32, smallest / len(cuts), top_value / len(cuts)))
        factor_of = factor_of * jnp.repeat(steps, shape[dim] // blocks).reshape([-1 if axis == dim else 1 for axis in range(len(shape))])
    return factor_of


def noise_with(own_key, shape, width, bound, split, heavy, held_as=jnp.bfloat16):
    array = width * jax.random.normal(own_key, shape, jnp.float32)
    if split:
        array = array * block_scale(own_key, shape, split, -0.22, 0.18)
    return jnp.clip(strengthened(array, jax.random.fold_in(own_key, 3), *heavy), -bound, bound).astype(held_as)


def setup_inputs(seed: int = 0) -> dict:
    splits = jax.random.split(jax.random.key(seed), 2)
    return {
        "source_blocks": noise_with(splits[0], (M, N), 1.0, 6.0, ((0, 4), (1, 8)), (0, 1, 8, 2.0), jnp.float32),
    }


def reference(source_blocks):
    row_count = N_ROW
    col_count = N_COL
    cells = source_blocks.reshape(row_count, M // row_count // SB, SB, col_count, N // col_count // SB, SB)
    matrix = cells.transpose(1, 0, 2, 4, 3, 5).reshape(M, N)
    pieces = matrix.reshape(RB, 2, 4, row_count // 4, TB, E, 2, col_count // 4, TB)
    target_blocks = pieces.transpose(3, 2, 0, 4, 7, 1, 6, 5, 8).reshape(M // 2, 2 * N)
    scale = 1.0 / math.sqrt(M)
    totals = lax.optimization_barrier(jnp.sum(matrix, axis=0)) * scale
    grouped = totals.reshape(E, 2, col_count // 4, TB).transpose(2, 1, 0, 3)
    column_sums = jnp.broadcast_to(grouped[:, None], (col_count // 4, 2, 2, E, TB)).reshape(2 * N)
    frobenius = jnp.sqrt(jnp.sum(matrix * matrix) / (M * N))
    return (target_blocks, column_sums, frobenius)
```

```python
import math

import jax
import jax.numpy as jnp
from jax import lax
from jax.experimental import pallas as pl
from jax.experimental.pallas import tpu as pltpu
from jax.sharding import Mesh
from jax.sharding import PartitionSpec as P

SB = 128
ROWS = 16
PEERS = ("r4", "zlo", "core")


def pack_kernel(source, packed, sums, squares):
    @pl.when(pl.program_id(0) == 0)
    def _():
        sums[...] = jnp.zeros_like(sums)
        squares[...] = jnp.zeros_like(squares)

    blocks = source.shape[3] // (2 * SB)
    square = squares[...]
    for e in range(blocks):
        for core in range(2):
            lanes = pl.ds((2 * e + core) * SB, SB)
            total = sums[:, lanes]
            for s in range(8):
                value = source[0, s, :, lanes]
                packed[(s % 4) * 4 + (s // 4) * 2 + core, :, pl.ds(e * SB, SB)] = value
                grouped = value.reshape(ROWS // 8, 8, SB)
                total = total + jnp.sum(grouped, axis=0)
                square = square + jnp.sum(grouped * grouped, axis=0)
            sums[:, lanes] = total
    squares[...] = square


def pack(source, part):
    cols = source.shape[3]
    return pl.pallas_call(
        pack_kernel,
        grid=(SB // ROWS,),
        in_specs=[pl.BlockSpec((1, 8, ROWS, cols), lambda j: (part, 0, j, 0))],
        out_specs=[
            pl.BlockSpec((16, ROWS, cols // 2), lambda j: (0, j, 0)),
            pl.BlockSpec((8, cols), lambda j: (0, 0)),
            pl.BlockSpec((8, SB), lambda j: (0, 0)),
        ],
        out_shape=[
            jax.ShapeDtypeStruct((16, SB, cols // 2), jnp.float32),
            jax.ShapeDtypeStruct((8, cols), jnp.float32),
            jax.ShapeDtypeStruct((8, SB), jnp.float32),
        ],
        cost_estimate=pl.CostEstimate(
            flops=2 * 10**9, bytes_accessed=64 * SB * cols, transcendentals=0
        ),
        name=f"pack_{part}",
    )(source)


def place_kernel(*refs):
    received, target = refs[0], refs[-1]
    for e in range(received.shape[2] // SB):
        for p in range(4):
            for q in range(4):
                target[0, p, :, pl.ds((4 * e + q) * SB, SB)] = received[
                    p * 4 + q, :, pl.ds(e * SB, SB)
                ]


def place(received, target, part, parts):
    width = received.shape[2] * 4
    more = [] if target is None else [target]
    return pl.pallas_call(
        place_kernel,
        grid=(SB // ROWS,),
        in_specs=[pl.BlockSpec((16, ROWS, width // 4), lambda j: (0, j, 0))]
        + [pl.BlockSpec(memory_space=pl.ANY) for _ in more],
        out_specs=pl.BlockSpec((1, 4, ROWS, width), lambda j: (part, 0, j, 0)),
        out_shape=jax.ShapeDtypeStruct((parts, 4, SB, width), jnp.float32),
        input_output_aliases={1: 0} if more else {},
        cost_estimate=pl.CostEstimate(
            flops=2 * 10**9, bytes_accessed=32 * SB * width, transcendentals=0
        ),
        name=f"place_{part}",
    )(received, *more)


def per_device(source_blocks):
    local_rows, local_cols = source_blocks.shape
    row_count = lax.axis_size(("rg", "r4"))
    col_count = lax.axis_size(("chi", "zlo", "core"))
    total_rows = local_rows * row_count
    total_cols = local_cols * col_count
    scale = 1.0 / math.sqrt(total_rows)
    parts = local_rows // (8 * SB)
    source = source_blocks.reshape(parts, 8, SB, local_cols)
    received, sums, squares = [], 0.0, 0.0
    for part in range(parts):
        packed, part_sums, part_squares = pack(source, part)
        sums = sums + part_sums
        squares = squares + part_squares
        received.append(
            lax.all_to_all(packed, PEERS, split_axis=0, concat_axis=0, tiled=True)
        )
    target = None
    for part in range(parts):
        target = place(received[part], target, part, parts)
    target_blocks = target.reshape(parts * 4 * SB, 2 * local_cols)

    sums = jnp.sum(sums, axis=0)
    squares = jnp.broadcast_to(jnp.sum(squares), (SB,))
    partial = lax.psum(jnp.concatenate([sums, squares]), ("rg", "r4"))
    every = lax.all_gather(partial, ("chi", "zlo", "core"))
    frobenius = jnp.sqrt(jnp.sum(every[:, local_cols]) / (total_rows * total_cols))
    mine = lax.dynamic_slice_in_dim(every, lax.axis_index("chi") * 4, 4, 0)
    mine = mine[:, :local_cols].reshape(4, local_cols // (2 * SB), 2, SB)
    mine = lax.dynamic_index_in_dim(mine, lax.axis_index("core"), 2, False)
    column_sums = mine.transpose(1, 0, 2).reshape(2 * local_cols) * scale
    return (target_blocks, column_sums, frobenius)


def solution(mesh):
    rows, cols = mesh.shape["row"], mesh.shape["col"]
    grid = Mesh(
        mesh.devices.reshape(rows // 4, 4, cols // 4, 2, 2),
        ("rg", "r4", "chi", "zlo", "core"),
    )
    row, col = ("rg", "r4"), ("chi", "zlo", "core")
    return jax.shard_map(
        per_device,
        mesh=grid,
        in_specs=(P(row, col),),
        out_specs=(P(row, col), P(col), P()),
        check_vma=False,
    )
```

```python
import math

import jax
import jax.numpy as jnp
from jax import lax
from jax.experimental import pallas as pl
from jax.sharding import Mesh
from jax.sharding import PartitionSpec as P

SB = 128
ROWS = 32
CHUNKS = 1
PEERS = ("r4", "zlo", "core")


def slab_rows(blocks):
    return (blocks // 8 + 1) * 8


def tree_sum(values):
    while len(values) > 1:
        values = [sum(values[i : i + 2]) for i in range(0, len(values), 2)]
    return values[0]


def pack_kernel(steps, tail, carried, *refs):
    source = refs[0]
    packed, sums, squares = refs[-3:]
    cols = source.shape[3]
    blocks = cols // (2 * SB)
    step = pl.program_id(0)

    @pl.when(step == 0)
    def _():
        if carried:
            sums[...] = refs[1][...]
            squares[...] = refs[2][...]
        else:
            sums[...] = jnp.zeros_like(sums)
            squares[...] = jnp.zeros_like(squares)

    @pl.when(step < steps)
    def _():
        square = [squares[...]] + [jnp.zeros((8, SB), jnp.float32)] * 3
        for e in range(blocks):
            for core in range(2):
                lanes = pl.ds((2 * e + core) * SB, SB)
                values = []
                for s in range(8):
                    peer = (s % 4) * 4 + (s // 4) * 2 + core
                    for o in range(ROWS // 8):
                        value = source[0, s, pl.ds(o * 8, 8), lanes]
                        packed[peer, pl.ds((o * blocks + e) * 8, 8), :] = value
                        values.append(value)
                for i in range(4):
                    square[i] = square[i] + tree_sum([v * v for v in values[i::4]])
                sums[:, lanes] = sums[:, lanes] + tree_sum(values)
        squares[...] = tree_sum(square)

    if tail:

        @pl.when(step == steps)
        def _():
            square = jnp.sum(squares[...], axis=0, keepdims=True)
            depth = slab_rows(blocks)
            for core in range(2):
                lines = [
                    jnp.sum(sums[:, pl.ds((2 * e + core) * SB, SB)], axis=0, keepdims=True)
                    for e in range(blocks)
                ]
                lines.append(square)
                lines.append(jnp.zeros((depth - blocks - 1, SB), jnp.float32))
                slab = jnp.concatenate([v for v in lines if v.shape[0]], axis=0)
                for peer in range(core, 16, 2):
                    packed[peer, pl.ds(0, depth), :] = slab


def pack(source, first, count, tail, carry):
    cols = source.shape[3]
    blocks = cols // (2 * SB)
    per = SB // ROWS
    steps = count * per
    depth = steps * ROWS * blocks + (slab_rows(blocks) if tail else 0)

    def at(j):
        j = jnp.minimum(j, steps - 1)
        return (first + j // per, 0, j % per, 0)

    whole = [
        pl.BlockSpec((8, cols), lambda j: (0, 0)),
        pl.BlockSpec((8, SB), lambda j: (0, 0)),
    ]
    return pl.pallas_call(
        lambda *refs: pack_kernel(steps, tail, bool(carry), *refs),
        grid=(steps + (1 if tail else 0),),
        in_specs=[pl.BlockSpec((1, 8, ROWS, cols), at)] + (whole if carry else []),
        out_specs=[
            pl.BlockSpec((16, ROWS * blocks, SB), lambda j: (0, j, 0)),
        ]
        + whole,
        out_shape=[
            jax.ShapeDtypeStruct((16, depth, SB), jnp.float32),
            jax.ShapeDtypeStruct((8, cols), jnp.float32),
            jax.ShapeDtypeStruct((8, SB), jnp.float32),
        ],
        cost_estimate=pl.CostEstimate(
            flops=2 * 10**9, bytes_accessed=64 * SB * cols, transcendentals=0
        ),
        name=f"pack_{first}",
    )(source, *carry)


def place_kernel(blocks, *refs):
    received, target = refs[0], refs[-1]
    for e in range(blocks):
        for p in range(4):
            for q in range(4):
                for o in range(ROWS // 8):
                    target[0, p, pl.ds(o * 8, 8), pl.ds((4 * e + q) * SB, SB)] = received[
                        p * 4 + q, pl.ds((o * blocks + e) * 8, 8), :
                    ]


def place(received, target, first, count, parts, blocks):
    width = blocks * 4 * SB
    per = SB // ROWS
    more = [] if target is None else [target]
    return pl.pallas_call(
        lambda *refs: place_kernel(blocks, *refs),
        grid=(count * per,),
        in_specs=[pl.BlockSpec((16, ROWS * blocks, SB), lambda j: (0, j, 0))]
        + [pl.BlockSpec(memory_space=pl.ANY) for _ in more],
        out_specs=pl.BlockSpec(
            (1, 4, ROWS, width), lambda j: (first + j // per, 0, j % per, 0)
        ),
        out_shape=jax.ShapeDtypeStruct((parts, 4, SB, width), jnp.float32),
        input_output_aliases={1: 0} if more else {},
        cost_estimate=pl.CostEstimate(
            flops=2 * 10**9, bytes_accessed=32 * SB * width, transcendentals=0
        ),
        name=f"place_{first}",
    )(received, *more)


def finish_kernel(blocks, scale, received, columns, squares):
    square = jnp.zeros((1, SB), jnp.float32)
    for q in range(4):
        total = tree_sum([received[p * 4 + q] for p in range(4)])
        for e in range(blocks):
            columns[pl.ds(4 * e + q, 1), :] = total[e : e + 1, :] * scale
        square = square + total[blocks : blocks + 1, :]
    squares[...] = square


def finish(received, blocks, scale):
    depth = slab_rows(blocks)
    last = received.shape[1] // depth - 1
    return pl.pallas_call(
        lambda *refs: finish_kernel(blocks, scale, *refs),
        grid=(1,),
        in_specs=[pl.BlockSpec((16, depth, SB), lambda j: (0, last, 0))],
        out_specs=[
            pl.BlockSpec((4 * blocks, SB), lambda j: (0, 0)),
            pl.BlockSpec((1, SB), lambda j: (0, 0)),
        ],
        out_shape=[
            jax.ShapeDtypeStruct((4 * blocks, SB), jnp.float32),
            jax.ShapeDtypeStruct((1, SB), jnp.float32),
        ],
        name="finish",
    )(received)


def per_device(source_blocks):
    local_rows, local_cols = source_blocks.shape
    row_count = lax.axis_size(("rg", "r4"))
    col_count = lax.axis_size(("chi", "zlo", "core"))
    total_rows = local_rows * row_count
    total_cols = local_cols * col_count
    blocks = local_cols // (2 * SB)
    parts = local_rows // (8 * SB)
    count = parts // CHUNKS
    source = source_blocks.reshape(parts, 8, SB, local_cols)
    received, carry = [], ()
    for first in range(0, parts, count):
        tail = first + count == parts
        packed, *carry = pack(source, first, count, tail, carry)
        received.append(
            lax.all_to_all(packed, PEERS, split_axis=0, concat_axis=0, tiled=True)
        )
    columns, squares = finish(received[-1], blocks, 1.0 / math.sqrt(total_rows))
    others = lax.axis_size(("rg", "chi"))
    total = squares
    for shift in range(1, others):
        pairs = [(i, (i + shift) % others) for i in range(others)]
        total = total + lax.ppermute(squares, ("rg", "chi"), pairs)
    if lax.axis_size("rg") > 1:
        columns = lax.psum(columns, "rg")
    target = None
    for i, first in enumerate(range(0, parts, count)):
        target = place(received[i], target, first, count, parts, blocks)
    target_blocks = target.reshape(parts * 4 * SB, 2 * local_cols)
    column_sums = columns.reshape(2 * local_cols)
    frobenius = jnp.sqrt(jnp.sum(total) / (total_rows * total_cols))
    return (target_blocks, column_sums, frobenius)


def solution(mesh):
    rows, cols = mesh.shape["row"], mesh.shape["col"]
    grid = Mesh(
        mesh.devices.reshape(rows // 4, 4, cols // 4, 2, 2),
        ("rg", "r4", "chi", "zlo", "core"),
    )
    row, col = ("rg", "r4"), ("chi", "zlo", "core")
    return jax.shard_map(
        per_device,
        mesh=grid,
        in_specs=(P(row, col),),
        out_specs=(P(row, col), P(col), P()),
        check_vma=False,
    )
```
